32 devices in a mesh: rows: 4 (over y, x), batch: 8 (over z, core).
Axes of the slice: x: 2, y: 2, z: 4, core: 2. Of those that a mesh axis runs over, the one named last changes fastest.
Arguments:
- control: bfloat16 [8, 24, 96, 320], P('batch', 'rows'), may hold values from -60 to 60, as said below
- unet_skips: bfloat16 [2, 8, 24, 96, 320], P(None, 'batch', 'rows'), may hold values from -6 to 6
- norm_gains: float32 [2, 2, 320], replicated, may hold values from 0.25 to 1.75
- norm_shifts: float32 [2, 2, 320], replicated, may hold values from -3 to 3
- conv_weights: bfloat16 [2, 2, 3, 960, 320], P(None, None, None, None, 'batch'), may hold values from -0.109375 to 0.109375
- zero_weights: bfloat16 [2, 1, 320, 320], P(None, None, None, 'batch'), may hold values from -0.3125 to 0.3125
Outputs:
- controls: bfloat16 [2, 8, 24, 96, 320], P(None, 'batch', 'rows')
The draws below stay inside these ranges and needn't reach their ends.
Inputs may be any that keep to these rules, and one draw needn't show every extreme that they name: `control`: Real-valued latent features.
All inputs are finite; a program needn't handle non-finite values.
Results may differ from the reference program's by a relative error of at most 0.01.
Values may be sent and summed in bfloat16 or wider, within the bound.
A program may use at most 64 MiB of HBM per device.

```python
import math
import jax
import jax.numpy as jnp
from jax import lax

C = 320
GROUPS = 32
W = 96
BLOCKS = 2
H = 24
BATCH = 8


def draw_control(key, part):
    first_key = jax.random.fold_in(jax.random.fold_in(key, 17), 0)
    second_key = jax.random.fold_in(jax.random.fold_in(key, 17), 1)
    fourth_key = jax.random.fold_in(jax.random.fold_in(key, 17), 3)
    row_pos = jnp.arange(H, dtype=jnp.float32) / max(H - 1, 1)
    channel_scale = jnp.exp(jax.random.uniform(second_key, (C,), jnp.float32, math.log(0.3), math.log(3.0)))
    channel_offset = jax.random.uniform(fourth_key, (C,), jnp.float32, 0.5, 1.5)
    base = jax.random.truncated_normal(first_key, -6.0, 6.0, (BATCH, H, W, C), jnp.float32)
    row_scale = 1.0 + 2.0 * row_pos
    ramp = 0.5 + 2.5 * row_pos
    values = base * row_scale[None, :, None, None] * channel_scale + ramp[None, :, None, None] * channel_offset
    return values.astype(jnp.bfloat16)


def steps_of(key, dims, cuts, low, largest):
    level = 1.0
    for position, blocks in cuts:
        draws = jax.random.uniform(jax.random.fold_in(jax.random.fold_in(key, 6), position), (blocks,), jnp.float32, low / len(cuts), largest / len(cuts))
        level = level * jnp.repeat(jnp.exp(draws), dims[position] // blocks).reshape((-1,) + (1,) * (len(dims) - 1 - position))
    return level


def gaussian(stream_key, dims, width, reach, cuts=(), kind=jnp.bfloat16):
    result = width * jax.random.normal(stream_key, dims, jnp.float32)
    if cuts:
        result = result * steps_of(stream_key, dims, cuts, -0.22, 0.18)
    return jnp.clip(result, -reach, reach).astype(kind)


def setup_inputs(seed: int = 0) -> dict:
    splits = jax.random.split(jax.random.key(seed), 7)
    return {
        "control": draw_control(jax.random.fold_in(splits[6], 71), 0),
        "unet_skips": gaussian(splits[1], (BLOCKS, BATCH, H, W, C), 1.0, 6.0, ((1, 8), (2, 4))),
        "norm_gains": jnp.clip(1.0 + 0.15 * jax.random.normal(splits[2], (BLOCKS, 2, C), jnp.float32), 0.25, 1.75),
        "norm_shifts": gaussian(splits[3], (BLOCKS, 2, C), 0.5, 3.0, (), jnp.float32),
        "conv_weights": gaussian(splits[4], (BLOCKS, 2, 3, 3 * C, C), (9 * C) ** -0.5, 0.109375, ((4, 8),)),
        "zero_weights": gaussian(splits[5], (BLOCKS, 1, C, C), C ** -0.5, 0.3125, ((3, 8),)),
    }


epsilon = 1e-05

def normalize(values, gain_row, shift_row):
    height, across, channels = values.shape
    grouped = values.astype(jnp.float32).reshape(height, across, GROUPS, channels // GROUPS)
    average = lax.optimization_barrier(jnp.mean(grouped, axis=(0, 1, 3), keepdims=True))
    centered = grouped - average
    spread = lax.optimization_barrier(jnp.mean(centered * centered, axis=(0, 1, 3), keepdims=True))
    scaled = (centered * lax.rsqrt(spread + epsilon)).reshape(height, across, channels) * gain_row + shift_row
    return jax.nn.silu(scaled).astype(jnp.bfloat16)

def convolve(values, weight):
    tap_rows = weight.shape[0]
    tap_cols = weight.shape[1] // values.shape[2]
    margin = tap_rows // 2
    height, across = (values.shape[0], values.shape[1])
    padded = jnp.pad(values, ((margin, margin), (margin, margin), (0, 0)))
    summed = jnp.zeros((height, across, weight.shape[2]), jnp.float32)
    for row_tap in range(tap_rows):
        row_band = padded[row_tap:row_tap + height]
        stacked = jnp.concatenate([row_band[:, col_tap:col_tap + across] for col_tap in range(tap_cols)], axis=2)
        summed = summed + jnp.einsum('hwk,kc->hwc', stacked.astype(jnp.float32), weight[row_tap].astype(jnp.float32))
    return summed

def reference(control, unet_skips, norm_gains, norm_shifts, conv_weights, zero_weights):

    def one_sample(inputs):
        hidden, skip_feats = inputs
        results = []
        for layer_index in range(conv_weights.shape[0]):
            normed = normalize(hidden, norm_gains[layer_index, 0], norm_shifts[layer_index, 0])
            first = convolve(normed, conv_weights[layer_index, 0]).astype(jnp.bfloat16)
            normed_two = normalize(first, norm_gains[layer_index, 1], norm_shifts[layer_index, 1])
            second = convolve(normed_two, conv_weights[layer_index, 1])
            hidden = (hidden.astype(jnp.float32) + second).astype(jnp.bfloat16)
            zeroed = convolve(hidden, zero_weights[layer_index])
            results.append((zeroed + skip_feats[layer_index].astype(jnp.float32)).astype(jnp.bfloat16))
        return jnp.stack(results)
    stacked_out = lax.map(one_sample, (control, jnp.moveaxis(unet_skips, 0, 1)))
    return jnp.moveaxis(stacked_out, 0, 1)
```

```python
import functools

import jax
import jax.numpy as jnp
import numpy as np
from jax import lax
from jax.experimental import pallas as pl
from jax.experimental.pallas import tpu as pltpu
from jax.sharding import PartitionSpec as P

GROUPS = 32
EPSILON = 1e-05
MESH = pl.DeviceIdType.MESH


def layout_of(conv_weights):
    blocks, convs, taps, depth, outs = conv_weights.shape
    channels = depth // 3
    places = convs * (depth // channels)
    need = taps * outs + -(-outs // places)
    lanes = -(-need // 128) * 128
    piece = min(outs, lanes - taps * outs)
    return lanes, piece, places


def packed(conv_weights, zero_weights):
    blocks, convs, taps, depth, outs = conv_weights.shape
    channels = zero_weights.shape[2]
    lanes, piece, places = layout_of(conv_weights)
    main = jnp.transpose(conv_weights, (0, 1, 3, 2, 4)).reshape(blocks, convs, depth, taps * outs)
    zero = zero_weights[:, 0]
    zero = jnp.pad(zero, ((0, 0), (0, 0), (0, places * piece - outs)))
    zero = jnp.transpose(zero.reshape(blocks, channels, places, piece), (0, 2, 1, 3))
    zero = zero.reshape(blocks, convs, depth, piece)
    slab = jnp.concatenate([main, zero], axis=3)
    slab = jnp.pad(slab, ((0, 0), (0, 0), (0, 0), (0, lanes - slab.shape[3])))
    return slab.reshape(blocks * convs, depth, lanes)


def kernel(dims, x_ref, skip_ref, gain_ref, shift_ref, group_ref, w_ref, out_ref,
           slabs, wfull, zfull, stk, halo, fields, acc, stat_out, stat_in,
           z_send, z_recv, a_send, a_recv, b_send, b_recv, d_send, d_recv,
           h_send, h_recv, t_send, t_recv):
    rows_n, batch_n, height, across, channels, outs, taps, piece, members = dims
    convs, depth, lanes = w_ref.shape
    zn = batch_n // 2
    r = lax.axis_index("rows")
    b = lax.axis_index("batch")
    z, c = b // 2, b % 2
    bit0, bit1 = r % 2, (r // 2) % 2
    px, py = r + 1 - 2 * bit0, r + 2 - 4 * bit1
    p1 = (1 - c) * px + c * py
    p2 = (1 - c) * py + c * px
    q = (1 - c) * (2 * bit1 + bit0) + c * (2 * bit0 + bit1)
    mate = b + 1 - 2 * c
    quarter, half = depth // 4, depth // 2
    mine = pl.ds(pl.multiple_of(q * quarter, quarter), quarter)
    peer = pl.ds(pl.multiple_of((q + 1 - 2 * (q % 2)) * quarter, quarter), quarter)
    my_half = pl.ds(pl.multiple_of((q // 2) * half, half), half)
    other_half = pl.ds(pl.multiple_of((1 - q // 2) * half, half), half)
    order = sorted(range(1, zn), key=lambda j: min(j, zn - j))

    def remote(src, dst, send, recv, row, batch):
        return pltpu.make_async_remote_copy(
            src_ref=src, dst_ref=dst, send_sem=send, recv_sem=recv,
            device_id={"rows": row, "batch": batch}, device_id_type=MESH)

    barrier = pltpu.get_barrier_semaphore()
    for j in range(1, zn):
        pl.semaphore_signal(barrier, inc=1, device_id_type=MESH,
                            device_id={"rows": r, "batch": ((z + j) % zn) * 2 + c})
    for j in range(1, rows_n):
        pl.semaphore_signal(barrier, inc=1, device_id_type=MESH,
                            device_id={"rows": (r + j) % rows_n, "batch": b})
    pl.semaphore_signal(barrier, inc=1, device_id_type=MESH, device_id={"rows": r, "batch": mate})
    pl.semaphore_wait(barrier, zn + rows_n - 1)

    sent = []

    def start(copy):
        copy.start()
        sent.append(copy)

    def source(j):
        return ((z + zn - j) % zn) * 2 + c

    def z_start(k):
        for j in order:
            start(remote(w_ref.at[k, mine], slabs.at[k, b, mine], z_send.at[k, j], z_recv.at[k, j],
                         r, ((z + j) % zn) * 2 + c))

    def a_step(k):
        for j in order:
            s = source(j)
            here = slabs.at[k, s, mine]
            remote(here, here, z_send.at[k, j], z_recv.at[k, j], p1, b).wait_recv()
            start(remote(here, here, a_send.at[k, j], a_recv.at[k, j], p1, b))

    def b_step(k):
        for j in order:
            s = source(j)
            got = slabs.at[k, s, peer]
            remote(got, got, a_send.at[k, j], a_recv.at[k, j], p1, b).wait_recv()
            here = slabs.at[k, s, my_half]
            start(remote(here, here, b_send.at[k, j], b_recv.at[k, j], p2, b))

    def d_step(k):
        for j in order:
            s = source(j)
            got = slabs.at[k, s, other_half]
            remote(got, got, b_send.at[k, j], b_recv.at[k, j], p2, b).wait_recv()
            here = slabs.at[k, s]
            start(remote(here, here, d_send.at[k, j], d_recv.at[k, j], r, mate))

    def d_wait(k):
        for j in [0] + order:
            s = ((z + zn - j) % zn) * 2 + (1 - c)
            here = slabs.at[k, s]
            remote(here, here, d_send.at[k, j], d_recv.at[k, j], r, mate).wait_recv()

    chunk = channels // 2

    def assemble(k):
        def body(i, carry):
            at = pl.multiple_of(i * chunk, chunk)
            parts = [slabs[k, d, pl.ds(at, chunk), :] for d in range(batch_n)]
            for tap in range(taps):
                wfull[tap, pl.ds(at, chunk), :] = jnp.concatenate(
                    [part[:, tap * outs:(tap + 1) * outs] for part in parts], axis=1)
            return carry
        lax.fori_loop(0, depth // chunk, body, 0)

    def assemble_zero(block):
        per = depth // channels
        for top in range(0, channels, chunk):
            parts = []
            for d in range(batch_n):
                for place in range(-(-outs // piece)):
                    k = block * (convs // (convs // 2)) + place // per
                    at = (place % per) * channels + top
                    wide = min(piece, outs - place * piece)
                    parts.append(slabs[k, d, at:at + chunk, taps * outs:taps * outs + wide])
            zfull[top:top + chunk, :] = jnp.concatenate(parts, axis=1)

    def halo_start(s, ref):
        cells = height * across

        def down():
            return remote(ref.at[pl.ds(cells - across, across)], halo.at[s, 0],
                          h_send.at[s, 0], h_recv.at[s, 0], (r + 1) % rows_n, b)

        def up():
            return remote(ref.at[pl.ds(0, across)], halo.at[s, 1],
                          h_send.at[s, 1], h_recv.at[s, 1], (r + rows_n - 1) % rows_n, b)

        @pl.when(r < rows_n - 1)
        def _():
            down().start()

        @pl.when(r > 0)
        def _():
            up().start()

        return down, up

    def stat_start(s, values):
        total = jnp.sum(values, axis=0, keepdims=True)
        square = jnp.sum(values * values, axis=0, keepdims=True)
        stat_out[s] = jnp.concatenate([total, square, jnp.zeros((6, channels), jnp.float32)], axis=0)
        for j in range(1, rows_n):
            start(remote(stat_out.at[s], stat_in.at[s, j], t_send.at[s, j], t_recv.at[s, j],
                         (r + j) % rows_n, b))

    col = lax.broadcasted_iota(jnp.int32, (across, channels), 0)

    def normalize(s, ref, ends):
        total = stat_out[s]
        for j in range(1, rows_n):
            here = stat_in.at[s, j]
            remote(here, here, t_send.at[s, j], t_recv.at[s, j], r, mate).wait_recv()
            total = total + stat_in[s, j]
        grouped = jnp.dot(total, group_ref[...], precision=lax.Precision.HIGHEST,
                          preferred_element_type=jnp.float32) * (1.0 / members)
        mean = grouped[0:1]
        spread = jnp.maximum(grouped[1:2] - mean * mean, 0.0)
        scale = lax.rsqrt(spread + EPSILON) * gain_ref[s:s + 1, :]
        bias = shift_ref[s:s + 1, :] - mean * scale

        def put(at, v, valid):
            y = v.astype(jnp.float32) * scale + bias
            a = y / (1.0 + jnp.exp(-y))
            if valid is not None:
                a = jnp.where(valid, a, 0.0)
            left = jnp.where(col == 0, 0.0, pltpu.roll(a, 1, 0))
            right = jnp.where(col == across - 1, 0.0, pltpu.roll(a, across - 1, 0))
            stk[pl.ds(at, across), :] = jnp.concatenate(
                [left.astype(jnp.bfloat16), a.astype(jnp.bfloat16), right.astype(jnp.bfloat16)], axis=1)

        def body(i, carry):
            at = pl.multiple_of(i * across, across)
            put(pl.multiple_of(at + across, across), ref[pl.ds(at, across), :], None)
            return carry
        lax.fori_loop(0, height, body, 0)
        down, up = ends

        @pl.when(r > 0)
        def _():
            down().wait_recv()

        @pl.when(r < rows_n - 1)
        def _():
            up().wait_recv()

        put(0, halo[s, 0], r > 0)
        put((height + 1) * across, halo[s, 1], r < rows_n - 1)

    def convolve():
        cells = height * across
        for tap in range(taps):
            part = jnp.dot(stk[tap * across:tap * across + cells, :], wfull[tap],
                           preferred_element_type=jnp.float32)
            if tap == 0:
                acc[...] = part
            elif tap < taps - 1:
                acc[...] += part
            else:
                return acc[...] + part

    ends = [halo_start(0, x_ref)]
    for k in range(convs):
        z_start(k)
        start(remote(w_ref.at[k], slabs.at[k, b], d_send.at[k, 0], d_recv.at[k, 0], r, mate))
    stat_start(0, x_ref[...].astype(jnp.float32))
    for k in range(convs):
        slabs[k, b] = w_ref[k]
    a_step(0)
    normalize(0, x_ref, ends[0])
    b_step(0)
    a_step(1)
    d_step(0)
    b_step(1)
    source_ref = x_ref
    for s in range(convs):
        d_wait(s)
        assemble(s)
        if s > 0:
            normalize(s, fields.at[s - 1], ends[s])
        result = convolve()
        if s % 2 == 0:
            fields[s] = result.astype(jnp.bfloat16)
        else:
            fields[s] = (source_ref[...].astype(jnp.float32) + result).astype(jnp.bfloat16)
            source_ref = fields.at[s]
        if s < convs - 1:
            ends.append(halo_start(s + 1, fields.at[s]))
            stat_start(s + 1, fields[s].astype(jnp.float32))
        if s + 2 < convs:
            a_step(s + 2)
        if s + 1 < convs:
            d_step(s + 1)
        if s + 2 < convs:
            b_step(s + 2)
        if s % 2 == 1:
            block = s // 2
            assemble_zero(block)
            zeroed = jnp.dot(fields[s], zfull[...], preferred_element_type=jnp.float32)
            out_ref[block] = (skip_ref[block].astype(jnp.float32) + zeroed).astype(jnp.bfloat16)
    for copy in sent:
        copy.wait_send()
    for down, up in ends:
        @pl.when(r < rows_n - 1)
        def _():
            down().wait_send()

        @pl.when(r > 0)
        def _():
            up().wait_send()


def on_device(rows_n, batch_n, control, unet_skips, norm_gains, norm_shifts, conv_weights, zero_weights):
    blocks, convs, taps, depth, outs = conv_weights.shape
    samples, height, across, channels = control.shape
    lanes, piece, places = layout_of(conv_weights)
    stages = blocks * convs
    cells = height * across
    per = channels // GROUPS
    member = np.arange(channels) // per
    group = jnp.asarray((member[:, None] == member[None, :]).astype(np.float32))
    slab = packed(conv_weights, zero_weights)
    members = cells * rows_n * per
    dims = (rows_n, batch_n, height, across, channels, outs, taps, piece, members)
    zn = batch_n // 2
    dma = pltpu.SemaphoreType.DMA
    vmem = pl.BlockSpec(memory_space=pltpu.VMEM)
    out = pl.pallas_call(
        functools.partial(kernel, dims),
        out_shape=jax.ShapeDtypeStruct((blocks, cells, channels), jnp.bfloat16),
        in_specs=[vmem] * 6,
        out_specs=vmem,
        scratch_shapes=[
            pltpu.VMEM((stages, batch_n, depth, lanes), jnp.bfloat16),
            pltpu.VMEM((taps, depth, channels), jnp.bfloat16),
            pltpu.VMEM((channels, channels), jnp.bfloat16),
            pltpu.VMEM(((height + taps - 1) * across, depth), jnp.bfloat16),
            pltpu.VMEM((stages, 2, across, channels), jnp.bfloat16),
            pltpu.VMEM((stages, cells, channels), jnp.bfloat16),
            pltpu.VMEM((cells, channels), jnp.float32),
            pltpu.VMEM((stages, 8, channels), jnp.float32),
            pltpu.VMEM((stages, rows_n, 8, channels), jnp.float32),
            dma((stages, zn)), dma((stages, zn)),
            dma((stages, zn)), dma((stages, zn)),
            dma((stages, zn)), dma((stages, zn)),
            dma((stages, zn)), dma((stages, zn)),
            dma((stages, 2)), dma((stages, 2)),
            dma((stages, rows_n)), dma((stages, rows_n)),
        ],
        compiler_params=pltpu.CompilerParams(
            collective_id=0, has_side_effects=True, vmem_limit_bytes=50 * 1024 * 1024),
    )(
        control.reshape(cells, channels),
        unet_skips.reshape(blocks, cells, channels),
        norm_gains.reshape(stages, channels),
        norm_shifts.reshape(stages, channels),
        group,
        slab,
    )
    return out.reshape(blocks, samples, height, across, channels)


def solution(mesh):
    placed = (
        P("batch", "rows", None, None),
        P(None, "batch", "rows", None, None),
        P(),
        P(),
        P(None, None, None, None, "batch"),
        P(None, None, None, "batch"),
    )
    return jax.shard_map(
        functools.partial(on_device, mesh.shape["rows"], mesh.shape["batch"]),
        mesh=mesh,
        in_specs=placed,
        out_specs=P(None, "batch", "rows", None, None),
        check_vma=False,
    )
```

```python
import functools

import jax
import jax.numpy as jnp
import numpy as np
from jax import lax
from jax.experimental import pallas as pl
from jax.experimental.pallas import tpu as pltpu
from jax.sharding import PartitionSpec as P

GROUPS = 32
EPSILON = 1e-05
MESH = pl.DeviceIdType.MESH


def transposed(conv_weights, zero_weights):
    blocks, convs, taps, depth, outs = conv_weights.shape
    conv = jnp.transpose(conv_weights, (0, 1, 2, 4, 3)).reshape(blocks * convs, taps * outs, depth)
    return conv, jnp.transpose(zero_weights[:, 0], (0, 2, 1))


def kernel(dims, x_ref, skip_ref, gain_ref, shift_ref, group_ref, w_ref, zw_ref, out_ref,
           slabs, wfull, zfull, stk, halo, fields, stat_out, stat_in,
           z_send, z_recv, a_send, a_recv, b_send, b_recv, d_send, d_recv,
           h_send, h_recv, t_send, t_recv):
    rows_n, batch_n, height, across, channels, outs, taps, members = dims
    convs, _, depth = w_ref.shape
    lanes = slabs.shape[3]
    piece = lanes - depth
    zn = batch_n // 2
    r = lax.axis_index("rows")
    b = lax.axis_index("batch")
    z, c = b // 2, b % 2
    bit0, bit1 = r % 2, (r // 2) % 2
    px, py = r + 1 - 2 * bit0, r + 2 - 4 * bit1
    p1 = (1 - c) * px + c * py
    p2 = (1 - c) * py + c * px
    q = (1 - c) * (2 * bit1 + bit0) + c * (2 * bit0 + bit1)
    mate = b + 1 - 2 * c
    quarter, half = lanes // 4, lanes // 2
    every = slice(None)
    mine = pl.ds(pl.multiple_of(q * quarter, quarter), quarter)
    peer = pl.ds(pl.multiple_of((q + 1 - 2 * (q % 2)) * quarter, quarter), quarter)
    my_half = pl.ds(pl.multiple_of((q // 2) * half, half), half)
    other_half = pl.ds(pl.multiple_of((1 - q // 2) * half, half), half)
    order = sorted(range(1, zn), key=lambda j: min(j, zn - j))

    def remote(src, dst, send, recv, row, batch):
        return pltpu.make_async_remote_copy(
            src_ref=src, dst_ref=dst, send_sem=send, recv_sem=recv,
            device_id={"rows": row, "batch": batch}, device_id_type=MESH)

    barrier = pltpu.get_barrier_semaphore()
    for j in range(1, zn):
        pl.semaphore_signal(barrier, inc=1, device_id_type=MESH,
                            device_id={"rows": r, "batch": ((z + j) % zn) * 2 + c})
    for j in range(1, rows_n):
        pl.semaphore_signal(barrier, inc=1, device_id_type=MESH,
                            device_id={"rows": (r + j) % rows_n, "batch": b})
    pl.semaphore_signal(barrier, inc=1, device_id_type=MESH, device_id={"rows": r, "batch": mate})

    pieces = -(-channels // piece)
    per_block = convs // zw_ref.shape[0]
    for k in range(convs):
        slabs[k, b, :, :depth] = w_ref[k]
        block = k // per_block
        for tap in range(taps):
            p = (k % per_block) * taps + tap
            if p < pieces:
                wide = min(piece, channels - p * piece)
                slabs[k, b, tap * outs:(tap + 1) * outs, depth:depth + wide] = (
                    zw_ref[block, :, p * piece:p * piece + wide])
    pl.semaphore_wait(barrier, zn + rows_n - 1)

    sent = []

    def start(copy):
        copy.start()
        sent.append(copy)

    def source(j):
        return ((z + zn - j) % zn) * 2 + c

    def z_start(k):
        here = slabs.at[k, b, every, mine]
        for j in order:
            start(remote(here, here, z_send.at[k, j], z_recv.at[k, j],
                         r, ((z + j) % zn) * 2 + c))

    def a_step(k):
        for j in order:
            s = source(j)
            here = slabs.at[k, s, every, mine]
            remote(here, here, z_send.at[k, j], z_recv.at[k, j], p1, b).wait_recv()
            start(remote(here, here, a_send.at[k, j], a_recv.at[k, j], p1, b))

    def b_step(k):
        for j in order:
            s = source(j)
            got = slabs.at[k, s, every, peer]
            remote(got, got, a_send.at[k, j], a_recv.at[k, j], p1, b).wait_recv()
            here = slabs.at[k, s, every, my_half]
            start(remote(here, here, b_send.at[k, j], b_recv.at[k, j], p2, b))

    def d_step(k):
        for j in order:
            s = source(j)
            got = slabs.at[k, s, every, other_half]
            remote(got, got, b_send.at[k, j], b_recv.at[k, j], p2, b).wait_recv()
            here = slabs.at[k, s]
            start(remote(here, here, d_send.at[k, j], d_recv.at[k, j], r, mate))

    def d_wait(k):
        for j in [0] + order:
            s = ((z + zn - j) % zn) * 2 + (1 - c)
            here = slabs.at[k, s]
            remote(here, here, d_send.at[k, j], d_recv.at[k, j], r, mate).wait_recv()

    def assemble(k):
        for d in range(batch_n):
            for tap in range(taps):
                wfull[tap, d * outs:(d + 1) * outs, :] = (
                    slabs[k, d, tap * outs:(tap + 1) * outs, :depth])

    def assemble_zero(block):
        for d in range(batch_n):
            parts = []
            for p in range(pieces):
                wide = min(piece, channels - p * piece)
                tap = p % taps
                parts.append(slabs[block * per_block + p // taps, d,
                                   tap * outs:(tap + 1) * outs, depth:depth + wide])
            zfull[d * outs:(d + 1) * outs, :] = jnp.concatenate(parts, axis=1)

    def times(a, w):
        return lax.dot_general(a, w, (((1,), (1,)), ((), ())), preferred_element_type=jnp.float32)

    def halo_start(s, ref):
        cells = height * across

        def down():
            return remote(ref.at[pl.ds(cells - across, across)], halo.at[s, 0],
                          h_send.at[s, 0], h_recv.at[s, 0], (r + 1) % rows_n, b)

        def up():
            return remote(ref.at[pl.ds(0, across)], halo.at[s, 1],
                          h_send.at[s, 1], h_recv.at[s, 1], (r + rows_n - 1) % rows_n, b)

        @pl.when(r < rows_n - 1)
        def _():
            down().start()

        @pl.when(r > 0)
        def _():
            up().start()

        return down, up

    def stat_start(s, total, square):
        stat_out[s] = jnp.concatenate([total, square, jnp.zeros((6, channels), jnp.float32)], axis=0)
        for j in range(1, rows_n):
            start(remote(stat_out.at[s], stat_in.at[s, j], t_send.at[s, j], t_recv.at[s, j],
                         (r + j) % rows_n, b))

    col = lax.broadcasted_iota(jnp.int32, (across, channels), 0)

    def normalize(s, ref):
        total = stat_out[s]
        for j in range(1, rows_n):
            here = stat_in.at[s, j]
            remote(here, here, t_send.at[s, j], t_recv.at[s, j], r, mate).wait_recv()
            total = total + stat_in[s, j]
        grouped = jnp.dot(total, group_ref[...], precision=lax.Precision.HIGHEST,
                          preferred_element_type=jnp.float32) * (1.0 / members)
        mean = grouped[0:1]
        spread = jnp.maximum(grouped[1:2] - mean * mean, 0.0)
        scale = lax.rsqrt(spread + EPSILON) * gain_ref[s:s + 1, :]
        bias = shift_ref[s:s + 1, :] - mean * scale

        def put(at, v, valid):
            y = v.astype(jnp.float32) * scale + bias
            a = y / (1.0 + jnp.exp(-y))
            if valid is not None:
                a = jnp.where(valid, a, 0.0)
            left = jnp.where(col == 0, 0.0, pltpu.roll(a, 1, 0))
            right = jnp.where(col == across - 1, 0.0, pltpu.roll(a, across - 1, 0))
            stk[pl.ds(at, across), :] = jnp.concatenate(
                [left.astype(jnp.bfloat16), a.astype(jnp.bfloat16), right.astype(jnp.bfloat16)], axis=1)

        def body(i, carry):
            at = pl.multiple_of(i * across, across)
            put(pl.multiple_of(at + across, across), ref[pl.ds(at, across), :], None)
            return carry
        lax.fori_loop(0, height, body, 0)
        return put

    def edges(s, put, ends):
        down, up = ends

        @pl.when(r > 0)
        def _():
            down().wait_recv()

        @pl.when(r < rows_n - 1)
        def _():
            up().wait_recv()

        put(0, halo[s, 0], r > 0)
        put((height + 1) * across, halo[s, 1], r < rows_n - 1)

    def inner():
        cells = (height - 2) * across
        total = None
        for tap in range(taps):
            at = (tap + 1) * across
            part = times(stk[at:at + cells, :], wfull[tap])
            total = part if total is None else total + part
        return total

    def outer():
        total = None
        for tap in range(taps):
            low, high = tap * across, (height - 1 + tap) * across
            both = jnp.concatenate([stk[low:low + across, :], stk[high:high + across, :]], axis=0)
            part = times(both, wfull[tap])
            total = part if total is None else total + part
        return total

    def convolve(s, put, ends, source):
        cells = height * across

        def keep(at, value):
            size = value.shape[0]
            if source is not None:
                value = source[at:at + size, :].astype(jnp.float32) + value
            value = value.astype(jnp.bfloat16)
            fields[s, at:at + size, :] = value
            kept = value.astype(jnp.float32)
            return (jnp.sum(kept, axis=0, keepdims=True),
                    jnp.sum(kept * kept, axis=0, keepdims=True))

        middle = keep(across, inner())
        edges(s, put, ends)
        border = outer()
        top = keep(0, border[:across])
        bottom = keep(cells - across, border[across:])
        return middle[0] + top[0] + bottom[0], middle[1] + top[1] + bottom[1]

    def zero_conv(s):
        block = s // per_block
        assemble_zero(block)
        zeroed = times(fields[s], zfull[...])
        out_ref[block] = (skip_ref[block].astype(jnp.float32) + zeroed).astype(jnp.bfloat16)

    ends = [halo_start(0, x_ref)]
    for k in range(convs):
        z_start(k)
        here = slabs.at[k, b]
        start(remote(here, here, d_send.at[k, 0], d_recv.at[k, 0], r, mate))
        if k == 0:
            first = x_ref[...].astype(jnp.float32)
            stat_start(0, jnp.sum(first, axis=0, keepdims=True),
                       jnp.sum(first * first, axis=0, keepdims=True))
    put = normalize(0, x_ref)
    a_step(0)
    b_step(0)
    a_step(1)
    d_step(0)
    b_step(1)
    source_ref = x_ref
    for s in range(convs):
        d_wait(s)
        assemble(s)
        if s + 2 < convs:
            a_step(s + 2)
        if s > 0:
            put = normalize(s, fields.at[s - 1])
        last = s % per_block == per_block - 1
        sums = convolve(s, put, ends[s], source_ref if last else None)
        if last:
            source_ref = fields.at[s]
        if s < convs - 1:
            stat_start(s + 1, *sums)
            ends.append(halo_start(s + 1, fields.at[s]))
        if s + 1 < convs:
            d_step(s + 1)
        if s + 2 < convs:
            b_step(s + 2)
        if last:
            zero_conv(s)
    for copy in sent:
        copy.wait_send()
    for down, up in ends:
        @pl.when(r < rows_n - 1)
        def _():
            down().wait_send()

        @pl.when(r > 0)
        def _():
            up().wait_send()


def on_device(rows_n, batch_n, control, unet_skips, norm_gains, norm_shifts, conv_weights, zero_weights):
    blocks, convs, taps, depth, outs = conv_weights.shape
    samples, height, across, channels = control.shape
    lanes = (depth // 512 + 1) * 512
    stages = blocks * convs
    cells = height * across
    per = channels // GROUPS
    member = np.arange(channels) // per
    group = jnp.asarray((member[:, None] == member[None, :]).astype(np.float32))
    conv, zero = transposed(conv_weights, zero_weights)
    members = cells * rows_n * per
    dims = (rows_n, batch_n, height, across, channels, outs, taps, members)
    zn = batch_n // 2
    dma = pltpu.SemaphoreType.DMA
    vmem = pl.BlockSpec(memory_space=pltpu.VMEM)
    out = pl.pallas_call(
        functools.partial(kernel, dims),
        out_shape=jax.ShapeDtypeStruct((blocks, cells, channels), jnp.bfloat16),
        in_specs=[vmem] * 7,
        out_specs=vmem,
        scratch_shapes=[
            pltpu.VMEM((stages, batch_n, taps * outs, lanes), jnp.bfloat16),
            pltpu.VMEM((taps, channels, depth), jnp.bfloat16),
            pltpu.VMEM((channels, channels), jnp.bfloat16),
            pltpu.VMEM(((height + taps - 1) * across, depth), jnp.bfloat16),
            pltpu.VMEM((stages, 2, across, channels), jnp.bfloat16),
            pltpu.VMEM((stages, cells, channels), jnp.bfloat16),
            pltpu.VMEM((stages, 8, channels), jnp.float32),
            pltpu.VMEM((stages, rows_n, 8, channels), jnp.float32),
            dma((stages, zn)), dma((stages, zn)),
            dma((stages, zn)), dma((stages, zn)),
            dma((stages, zn)), dma((stages, zn)),
            dma((stages, zn)), dma((stages, zn)),
            dma((stages, 2)), dma((stages, 2)),
            dma((stages, rows_n)), dma((stages, rows_n)),
        ],
        compiler_params=pltpu.CompilerParams(
            collective_id=0, has_side_effects=True, vmem_limit_bytes=50 * 1024 * 1024),
    )(
        control.reshape(cells, channels),
        unet_skips.reshape(blocks, cells, channels),
        norm_gains.reshape(stages, channels),
        norm_shifts.reshape(stages, channels),
        group,
        conv,
        zero,
    )
    return out.reshape(blocks, samples, height, across, channels)


def solution(mesh):
    placed = (
        P("batch", "rows", None, None),
        P(None, "batch", "rows", None, None),
        P(),
        P(),
        P(None, None, None, None, "batch"),
        P(None, None, None, "batch"),
    )
    return jax.shard_map(
        functools.partial(on_device, mesh.shape["rows"], mesh.shape["batch"]),
        mesh=mesh,
        in_specs=placed,
        out_specs=P(None, "batch", "rows", None, None),
        check_vma=False,
    )
```

```python
import functools

import jax
import jax.numpy as jnp
import numpy as np
from jax import lax
from jax.experimental import pallas as pl
from jax.experimental.pallas import tpu as pltpu
from jax.sharding import PartitionSpec as P

GROUPS = 32
EPSILON = 1e-05
MESH = pl.DeviceIdType.MESH


def transposed(conv_weights, zero_weights):
    blocks, convs, taps, depth, outs = conv_weights.shape
    conv = jnp.transpose(conv_weights, (0, 1, 2, 4, 3)).reshape(blocks * convs, taps * outs, depth)
    return conv, jnp.transpose(zero_weights[:, 0], (0, 2, 1))


def kernel(dims, x_far, skip_far, gain_far, shift_far, group_far, w_far, zw_far, out_ref,
           x_ref, skip_ref, gain_ref, shift_ref, group_ref, w_ref, zw_ref, near_sem,
           slabs, wfull, zfull, stk, halo, fields, stat_out, stat_in,
           z_send, z_recv, a_send, a_recv, b_send, b_recv, d_send, d_recv,
           h_send, h_recv, t_send, t_recv):
    rows_n, batch_n, height, across, channels, outs, taps, members = dims
    convs, _, depth = w_ref.shape
    loads = [pltpu.make_async_copy(far, close, near_sem.at[i]) for i, (far, close) in enumerate((
        (w_far, w_ref), (zw_far, zw_ref), (x_far, x_ref), (gain_far, gain_ref),
        (shift_far, shift_ref), (group_far, group_ref), (skip_far, skip_ref)))]
    for load in loads:
        load.start()
    lanes = slabs.shape[3]
    piece = lanes - depth
    zn = batch_n // 2
    r = lax.axis_index("rows")
    b = lax.axis_index("batch")
    z, c = b // 2, b % 2
    bit0, bit1 = r % 2, (r // 2) % 2
    px, py = r + 1 - 2 * bit0, r + 2 - 4 * bit1
    p1 = (1 - c) * px + c * py
    p2 = (1 - c) * py + c * px
    q = (1 - c) * (2 * bit1 + bit0) + c * (2 * bit0 + bit1)
    mate = b + 1 - 2 * c
    quarter, half = lanes // 4, lanes // 2
    every = slice(None)
    mine = pl.ds(pl.multiple_of(q * quarter, quarter), quarter)
    peer = pl.ds(pl.multiple_of((q + 1 - 2 * (q % 2)) * quarter, quarter), quarter)
    my_half = pl.ds(pl.multiple_of((q // 2) * half, half), half)
    other_half = pl.ds(pl.multiple_of((1 - q // 2) * half, half), half)
    order = sorted(range(1, zn), key=lambda j: min(j, zn - j))

    def remote(src, dst, send, recv, row, batch):
        return pltpu.make_async_remote_copy(
            src_ref=src, dst_ref=dst, send_sem=send, recv_sem=recv,
            device_id={"rows": row, "batch": batch}, device_id_type=MESH)

    barrier = pltpu.get_barrier_semaphore()
    for j in range(1, zn):
        pl.semaphore_signal(barrier, inc=1, device_id_type=MESH,
                            device_id={"rows": r, "batch": ((z + j) % zn) * 2 + c})
    for j in range(1, rows_n):
        pl.semaphore_signal(barrier, inc=1, device_id_type=MESH,
                            device_id={"rows": (r + j) % rows_n, "batch": b})
    pl.semaphore_signal(barrier, inc=1, device_id_type=MESH, device_id={"rows": r, "batch": mate})

    for load in loads[:-1]:
        load.wait()
    pieces = -(-channels // piece)
    per_block = convs // zw_ref.shape[0]
    for k in range(convs):
        slabs[k, b, :, :depth] = w_ref[k]
        block = k // per_block
        for tap in range(taps):
            p = (k % per_block) * taps + tap
            if p < pieces:
                wide = min(piece, channels - p * piece)
                slabs[k, b, tap * outs:(tap + 1) * outs, depth:depth + wide] = (
                    zw_ref[block, :, p * piece:p * piece + wide])
    pl.semaphore_wait(barrier, zn + rows_n - 1)

    sent = []

    def start(copy):
        copy.start()
        sent.append(copy)

    def source(j):
        return ((z + zn - j) % zn) * 2 + c

    def z_start(k):
        here = slabs.at[k, b, every, mine]
        for j in order:
            start(remote(here, here, z_send.at[k, j], z_recv.at[k, j],
                         r, ((z + j) % zn) * 2 + c))

    def a_step(k):
        for j in order:
            s = source(j)
            here = slabs.at[k, s, every, mine]
            remote(here, here, z_send.at[k, j], z_recv.at[k, j], p1, b).wait_recv()
            start(remote(here, here, a_send.at[k, j], a_recv.at[k, j], p1, b))

    def b_step(k):
        for j in order:
            s = source(j)
            got = slabs.at[k, s, every, peer]
            remote(got, got, a_send.at[k, j], a_recv.at[k, j], p1, b).wait_recv()
            here = slabs.at[k, s, every, my_half]
            start(remote(here, here, b_send.at[k, j], b_recv.at[k, j], p2, b))

    def d_step(k):
        for j in order:
            s = source(j)
            got = slabs.at[k, s, every, other_half]
            remote(got, got, b_send.at[k, j], b_recv.at[k, j], p2, b).wait_recv()
            here = slabs.at[k, s]
            start(remote(here, here, d_send.at[k, j], d_recv.at[k, j], r, mate))

    def d_wait(k):
        for j in [0] + order:
            s = ((z + zn - j) % zn) * 2 + (1 - c)
            here = slabs.at[k, s]
            remote(here, here, d_send.at[k, j], d_recv.at[k, j], r, mate).wait_recv()

    def assemble(k):
        for d in range(batch_n):
            for tap in range(taps):
                wfull[tap, d * outs:(d + 1) * outs, :] = (
                    slabs[k, d, tap * outs:(tap + 1) * outs, :depth])

    def assemble_zero(block):
        for d in range(batch_n):
            parts = []
            for p in range(pieces):
                wide = min(piece, channels - p * piece)
                tap = p % taps
                parts.append(slabs[block * per_block + p // taps, d,
                                   tap * outs:(tap + 1) * outs, depth:depth + wide])
            zfull[d * outs:(d + 1) * outs, :] = jnp.concatenate(parts, axis=1)

    def times(a, w):
        return lax.dot_general(a, w, (((1,), (1,)), ((), ())), preferred_element_type=jnp.float32)

    def halo_start(s, ref):
        cells = height * across

        def down():
            return remote(ref.at[pl.ds(cells - across, across)], halo.at[s, 0],
                          h_send.at[s, 0], h_recv.at[s, 0], (r + 1) % rows_n, b)

        def up():
            return remote(ref.at[pl.ds(0, across)], halo.at[s, 1],
                          h_send.at[s, 1], h_recv.at[s, 1], (r + rows_n - 1) % rows_n, b)

        @pl.when(r < rows_n - 1)
        def _():
            down().start()

        @pl.when(r > 0)
        def _():
            up().start()

        return down, up

    def stat_start(s, total, square):
        stat_out[s] = jnp.concatenate([total, square, jnp.zeros((6, channels), jnp.float32)], axis=0)
        for j in range(1, rows_n):
            start(remote(stat_out.at[s], stat_in.at[s, j], t_send.at[s, j], t_recv.at[s, j],
                         (r + j) % rows_n, b))

    col = lax.broadcasted_iota(jnp.int32, (across, channels), 0)

    def normalize(s, ref):
        total = stat_out[s]
        for j in range(1, rows_n):
            here = stat_in.at[s, j]
            remote(here, here, t_send.at[s, j], t_recv.at[s, j], r, mate).wait_recv()
            total = total + stat_in[s, j]
        grouped = jnp.dot(total, group_ref[...], precision=lax.Precision.HIGHEST,
                          preferred_element_type=jnp.float32) * (1.0 / members)
        mean = grouped[0:1]
        spread = jnp.maximum(grouped[1:2] - mean * mean, 0.0)
        scale = lax.rsqrt(spread + EPSILON) * gain_ref[s // per_block, s % per_block:s % per_block + 1, :]
        bias = shift_ref[s // per_block, s % per_block:s % per_block + 1, :] - mean * scale

        def put(at, v, valid):
            y = v.astype(jnp.float32) * scale + bias
            a = y / (1.0 + jnp.exp(-y))
            if valid is not None:
                a = jnp.where(valid, a, 0.0)
            left = jnp.where(col == 0, 0.0, pltpu.roll(a, 1, 0))
            right = jnp.where(col == across - 1, 0.0, pltpu.roll(a, across - 1, 0))
            stk[pl.ds(at, across), :] = jnp.concatenate(
                [left.astype(jnp.bfloat16), a.astype(jnp.bfloat16), right.astype(jnp.bfloat16)], axis=1)

        def body(i, carry):
            at = pl.multiple_of(i * across, across)
            put(pl.multiple_of(at + across, across), ref[pl.ds(at, across), :], None)
            return carry
        lax.fori_loop(0, height, body, 0)
        return put

    def edges(s, put, ends):
        down, up = ends

        @pl.when(r > 0)
        def _():
            down().wait_recv()

        @pl.when(r < rows_n - 1)
        def _():
            up().wait_recv()

        put(0, halo[s, 0], r > 0)
        put((height + 1) * across, halo[s, 1], r < rows_n - 1)

    def inner():
        cells = (height - 2) * across
        total = None
        for tap in range(taps):
            at = (tap + 1) * across
            part = times(stk[at:at + cells, :], wfull[tap])
            total = part if total is None else total + part
        return total

    def outer():
        total = None
        for tap in range(taps):
            low, high = tap * across, (height - 1 + tap) * across
            both = jnp.concatenate([stk[low:low + across, :], stk[high:high + across, :]], axis=0)
            part = times(both, wfull[tap])
            total = part if total is None else total + part
        return total

    def convolve(s, put, ends, source):
        cells = height * across

        def keep(at, value):
            size = value.shape[0]
            if source is not None:
                value = source[at:at + size, :].astype(jnp.float32) + value
            value = value.astype(jnp.bfloat16)
            fields[s, at:at + size, :] = value
            kept = value.astype(jnp.float32)
            return (jnp.sum(kept, axis=0, keepdims=True),
                    jnp.sum(kept * kept, axis=0, keepdims=True))

        middle = keep(across, inner())
        edges(s, put, ends)
        border = outer()
        top = keep(0, border[:across])
        bottom = keep(cells - across, border[across:])
        return middle[0] + top[0] + bottom[0], middle[1] + top[1] + bottom[1]

    def zero_conv(s):
        block = s // per_block
        assemble_zero(block)
        zeroed = times(fields[s], zfull[...])
        out_ref[block] = (skip_ref[block].astype(jnp.float32) + zeroed).astype(jnp.bfloat16)

    ends = [halo_start(0, x_ref)]
    for k in range(convs):
        z_start(k)
        here = slabs.at[k, b]
        start(remote(here, here, d_send.at[k, 0], d_recv.at[k, 0], r, mate))
        if k == 0:
            first = x_ref[...].astype(jnp.float32)
            stat_start(0, jnp.sum(first, axis=0, keepdims=True),
                       jnp.sum(first * first, axis=0, keepdims=True))
    put = normalize(0, x_ref)
    a_step(0)
    b_step(0)
    a_step(1)
    d_step(0)
    b_step(1)
    loads[-1].wait()
    source_ref = x_ref
    for s in range(convs):
        d_wait(s)
        assemble(s)
        if s + 2 < convs:
            a_step(s + 2)
        if s > 0:
            put = normalize(s, fields.at[s - 1])
        last = s % per_block == per_block - 1
        sums = convolve(s, put, ends[s], source_ref if last else None)
        if last:
            source_ref = fields.at[s]
        if s < convs - 1:
            stat_start(s + 1, *sums)
            ends.append(halo_start(s + 1, fields.at[s]))
        if s + 1 < convs:
            d_step(s + 1)
        if s + 2 < convs:
            b_step(s + 2)
        if last:
            zero_conv(s)
    for copy in sent:
        copy.wait_send()
    for down, up in ends:
        @pl.when(r < rows_n - 1)
        def _():
            down().wait_send()

        @pl.when(r > 0)
        def _():
            up().wait_send()


def on_device(rows_n, batch_n, control, unet_skips, norm_gains, norm_shifts, conv_weights, zero_weights):
    blocks, convs, taps, depth, outs = conv_weights.shape
    samples, height, across, channels = control.shape
    lanes = (depth // 512 + 1) * 512
    stages = blocks * convs
    cells = height * across
    per = channels // GROUPS
    member = np.arange(channels) // per
    group = jnp.asarray((member[:, None] == member[None, :]).astype(np.float32))
    conv, zero = transposed(conv_weights, zero_weights)
    members = cells * rows_n * per
    dims = (rows_n, batch_n, height, across, channels, outs, taps, members)
    zn = batch_n // 2
    dma = pltpu.SemaphoreType.DMA
    vmem = pl.BlockSpec(memory_space=pltpu.VMEM)
    out = pl.pallas_call(
        functools.partial(kernel, dims),
        out_shape=jax.ShapeDtypeStruct((blocks, cells, channels), jnp.bfloat16),
        in_specs=[pl.BlockSpec(memory_space=pltpu.HBM)] * 7,
        out_specs=vmem,
        scratch_shapes=[
            pltpu.VMEM((cells, channels), jnp.bfloat16),
            pltpu.VMEM((blocks, cells, channels), jnp.bfloat16),
            pltpu.VMEM(norm_gains.shape, jnp.float32),
            pltpu.VMEM(norm_shifts.shape, jnp.float32),
            pltpu.VMEM(group.shape, jnp.float32),
            pltpu.VMEM(conv.shape, jnp.bfloat16),
            pltpu.VMEM(zero.shape, jnp.bfloat16),
            dma((7,)),
            pltpu.VMEM((stages, batch_n, taps * outs, lanes), jnp.bfloat16),
            pltpu.VMEM((taps, channels, depth), jnp.bfloat16),
            pltpu.VMEM((channels, channels), jnp.bfloat16),
            pltpu.VMEM(((height + taps - 1) * across, depth), jnp.bfloat16),
            pltpu.VMEM((stages, 2, across, channels), jnp.bfloat16),
            pltpu.VMEM((stages, cells, channels), jnp.bfloat16),
            pltpu.VMEM((stages, 8, channels), jnp.float32),
            pltpu.VMEM((stages, rows_n, 8, channels), jnp.float32),
            dma((stages, zn)), dma((stages, zn)),
            dma((stages, zn)), dma((stages, zn)),
            dma((stages, zn)), dma((stages, zn)),
            dma((stages, zn)), dma((stages, zn)),
            dma((stages, 2)), dma((stages, 2)),
            dma((stages, rows_n)), dma((stages, rows_n)),
        ],
        compiler_params=pltpu.CompilerParams(
            collective_id=0, has_side_effects=True, vmem_limit_bytes=50 * 1024 * 1024),
    )(
        control.reshape(cells, channels),
        unet_skips.reshape(blocks, cells, channels),
        norm_gains,
        norm_shifts,
        group,
        conv,
        zero,
    )
    return out.reshape(blocks, samples, height, across, channels)


def solution(mesh):
    placed = (
        P("batch", "rows", None, None),
        P(None, "batch", "rows", None, None),
        P(),
        P(),
        P(None, None, None, None, "batch"),
        P(None, None, None, "batch"),
    )
    return jax.shard_map(
        functools.partial(on_device, mesh.shape["rows"], mesh.shape["batch"]),
        mesh=mesh,
        in_specs=placed,
        out_specs=P(None, "batch", "rows", None, None),
        check_vma=False,
    )
```
